32 devices in a mesh: kt: 8 (over z, y), tile: 4 (over x, core).
Axes of the slice: x: 2, y: 2, z: 4, core: 2. Of those that a mesh axis runs over, the one named last changes fastest.
Arguments:
- green_particle: bfloat16 [2, 64, 1024, 1024], P(None, 'kt', 'tile'), may hold values from -6 to 6
- green_hole: bfloat16 [2, 64, 1024, 1024], P(None, 'kt', 'tile'), may hold values from -6 to 6
- coulomb: bfloat16 [2, 64, 1024, 1024], P(None, 'kt'), may hold values from -3 to 3
Outputs:
- screened: float32 [2, 64, 1024, 1024], P(None, 'kt', 'tile')
The draws below stay inside these ranges and needn't reach their ends.
All inputs are finite; a program needn't handle non-finite values.
Results may differ from the reference program's by a relative error of at most 0.0039.
Values may be sent and summed in bfloat16 or wider, within the bound.
No kernel may reach another device: no remote copies, remote signals or barrier semaphores. Data moves between devices by JAX's collectives and lax.ppermute only.
A program may use at most 192 MiB of HBM per device.

```python
import math
import jax
import jax.numpy as jnp
from jax import lax

KSIDE = 4
NAO = 1024
K = 64


def shard_levels(key, shape, pieces, least, largest):
    def one(position, parts):
        draws = jax.random.uniform(jax.random.fold_in(jax.random.fold_in(key, 6), position), (parts,), jnp.float32, least / len(pieces), largest / len(pieces))
        return jnp.repeat(jnp.exp(draws), shape[position] // parts).reshape((-1,) + (1,) * (len(shape) - position - 1))

    factor_of = one(*pieces[0])
    for cut in pieces[1:]:
        factor_of = factor_of * one(*cut)
    return factor_of


def scatter_about(stream_key, shape, scale, reach, pieces=(), held_as=jnp.bfloat16):
    entries = jax.random.normal(stream_key, shape, jnp.float32) * scale
    if len(pieces) > 0:
        entries = shard_levels(stream_key, shape, pieces, -0.22, 0.18) * entries
    return jnp.clip(entries, min=-reach, max=reach).astype(held_as)


def setup_inputs(seed: int = 0) -> dict:
    streams_of = jax.random.split(jax.random.key(seed), 4)
    green_particle = scatter_about(streams_of[0], (2, K, NAO, NAO), 1.0, 6.0, ((1, 8), (2, 4)))
    green_hole = scatter_about(streams_of[1], (2, K, NAO, NAO), 1.0, 6.0, ((1, 8), (2, 4)))
    coulomb = scatter_about(streams_of[2], (2, K, NAO, NAO), 0.5, 3.0, ((1, 8),))
    return {"green_particle": green_particle, "green_hole": green_hole, "coulomb": coulomb}


HIGHEST = lax.Precision.HIGHEST


def phase_tables():
    point_index = jnp.arange(K, dtype=jnp.int32)
    digit_high = point_index // (KSIDE * KSIDE)
    digit_mid = (point_index // KSIDE) % KSIDE
    digit_low = point_index % KSIDE
    phase_turns = (digit_high[:, None] * digit_high[None, :] + digit_mid[:, None] * digit_mid[None, :] + digit_low[:, None] * digit_low[None, :]) % KSIDE
    angles = phase_turns.astype(jnp.float32) * (2.0 * math.pi / KSIDE)
    return jnp.cos(angles) / K, jnp.sin(angles) / K


def to_cells(real_part, imag_part, cosine_table, sine_table):
    return (jnp.dot(cosine_table, real_part, precision=HIGHEST) - jnp.dot(sine_table, imag_part, precision=HIGHEST),
            jnp.dot(sine_table, real_part, precision=HIGHEST) + jnp.dot(cosine_table, imag_part, precision=HIGHEST))


def to_momenta(real_part, imag_part, cosine_table, sine_table):
    return (jnp.dot(cosine_table, real_part, precision=HIGHEST) + jnp.dot(sine_table, imag_part, precision=HIGHEST),
            jnp.dot(cosine_table, imag_part, precision=HIGHEST) - jnp.dot(sine_table, real_part, precision=HIGHEST))


def polarize(particle, hole_part):
    cosine_table, sine_table = phase_tables()
    part_real, part_imag = to_cells(particle[0].astype(jnp.float32), particle[1].astype(jnp.float32), cosine_table, sine_table)
    hole_real, hole_imag = to_cells(hole_part[0].astype(jnp.float32), hole_part[1].astype(jnp.float32), cosine_table, sine_table)
    cell_real = part_real * hole_real - part_imag * hole_imag
    cell_imag = part_real * hole_imag + part_imag * hole_real
    mom_real, mom_imag = to_momenta(cell_real, cell_imag, cosine_table, sine_table)
    return jnp.stack([mom_real, mom_imag]).astype(jnp.bfloat16)


def complex_product(left_real, left_imag, right_real, right_imag):
    real_out = jnp.dot(left_real, right_real, preferred_element_type=jnp.float32) - jnp.dot(left_imag, right_imag, preferred_element_type=jnp.float32)
    imag_out = jnp.dot(left_real, right_imag, preferred_element_type=jnp.float32) + jnp.dot(left_imag, right_real, preferred_element_type=jnp.float32)
    return real_out, imag_out


def reference(green_particle, green_hole, coulomb):
    blocks = NAO // 64
    split_part = green_particle.reshape(2, K, blocks, 64, NAO).transpose(2, 0, 1, 3, 4)
    split_hole = green_hole.reshape(2, K, blocks, 64, NAO).transpose(2, 0, 1, 3, 4)

    def polarize_block(inputs_pair):
        result = polarize(inputs_pair[0].reshape(2, K, 64 * NAO), inputs_pair[1].reshape(2, K, 64 * NAO))
        return result.reshape(2, K, 64, NAO)

    polar_q = lax.map(polarize_block, (split_part, split_hole))
    polar_q = polar_q.transpose(1, 2, 0, 3, 4).reshape(2, K, NAO, NAO)

    def screen(inputs_pair):
        polar_k, coulomb_k = inputs_pair
        prod_real, prod_imag = complex_product(polar_k[0], polar_k[1], coulomb_k[0], coulomb_k[1])
        mid_real = prod_real.astype(jnp.bfloat16)
        mid_imag = prod_imag.astype(jnp.bfloat16)
        out_real, out_imag = complex_product(coulomb_k[0], coulomb_k[1], mid_real, mid_imag)
        return jnp.stack([coulomb_k[0].astype(jnp.float32) + out_real, coulomb_k[1].astype(jnp.float32) + out_imag])

    screened = lax.map(screen, (polar_q.transpose(1, 0, 2, 3), coulomb.transpose(1, 0, 2, 3)))
    return screened.transpose(1, 0, 2, 3)
```

```python
import math

import jax
import jax.numpy as jnp
from jax import lax
from jax.experimental import pallas as pl
from jax.experimental.pallas import tpu as pltpu
from jax.sharding import PartitionSpec as P


KSIDE = 4
LANES = 128
SUB = 16


HIGHEST = lax.Precision.HIGHEST


def phase_tables(points, side_count):
    point_index = jnp.arange(points, dtype=jnp.int32)
    digit_high = point_index // (side_count * side_count)
    digit_mid = point_index // side_count % side_count
    digit_low = point_index % side_count
    phase_turns = (
        digit_high[:, None] * digit_high[None, :]
        + digit_mid[:, None] * digit_mid[None, :]
        + digit_low[:, None] * digit_low[None, :]
    ) % side_count
    angles = phase_turns.astype(jnp.float32) * (2.0 * math.pi / side_count)
    return (jnp.cos(angles) / points, jnp.sin(angles) / points)


def to_cells(real_part, imag_part, cosine_table, sine_table):
    return (
        jnp.dot(cosine_table, real_part, precision=HIGHEST)
        - jnp.dot(sine_table, imag_part, precision=HIGHEST),
        jnp.dot(sine_table, real_part, precision=HIGHEST)
        + jnp.dot(cosine_table, imag_part, precision=HIGHEST),
    )


def to_momenta(real_part, imag_part, cosine_table, sine_table):
    return (
        jnp.dot(cosine_table, real_part, precision=HIGHEST)
        + jnp.dot(sine_table, imag_part, precision=HIGHEST),
        jnp.dot(cosine_table, imag_part, precision=HIGHEST)
        - jnp.dot(sine_table, real_part, precision=HIGHEST),
    )


def polarize(particle, hole_part):
    cosine_table, sine_table = phase_tables(particle.shape[1], KSIDE)
    part_real, part_imag = to_cells(
        particle[0].astype(jnp.float32), particle[1].astype(jnp.float32), cosine_table, sine_table
    )
    hole_real, hole_imag = to_cells(
        hole_part[0].astype(jnp.float32), hole_part[1].astype(jnp.float32), cosine_table, sine_table
    )
    cell_real = part_real * hole_real - part_imag * hole_imag
    cell_imag = part_real * hole_imag + part_imag * hole_real
    mom_real, mom_imag = to_momenta(cell_real, cell_imag, cosine_table, sine_table)
    return jnp.stack([mom_real, mom_imag]).astype(jnp.bfloat16)


def product_of(left_side, right_side):
    return jnp.einsum("kij,kjl->kil", left_side, right_side, preferred_element_type=jnp.float32)


def complex_batched(left_real, left_imag, right_real, right_imag):
    real_out = product_of(left_real, right_real) - product_of(left_imag, right_imag)
    imag_out = product_of(left_real, right_imag) + product_of(left_imag, right_real)
    return (real_out, imag_out)


def generic_body(green_particle, green_hole, coulomb):
    tile_rows = green_particle.shape[2]
    moved_part, moved_hole = (
        lax.all_to_all(green_particle, "kt", split_axis=3, concat_axis=1, tiled=True),
        lax.all_to_all(green_hole, "kt", split_axis=3, concat_axis=1, tiled=True),
    )
    points = moved_part.shape[1]
    narrow = moved_part.shape[3]
    polar_q = polarize(
        moved_part.reshape(2, points, tile_rows * narrow),
        moved_hole.reshape(2, points, tile_rows * narrow),
    )
    polar_q = polar_q.reshape(2, points, tile_rows, narrow)
    polar_rows = lax.all_to_all(polar_q, "kt", split_axis=1, concat_axis=3, tiled=True)
    mid_real, mid_imag = complex_batched(polar_rows[0], polar_rows[1], coulomb[0], coulomb[1])
    mid_stack = jnp.stack([mid_real.astype(jnp.bfloat16), mid_imag.astype(jnp.bfloat16)])
    row_start = lax.axis_index("tile") * tile_rows
    coulomb_rows = lax.dynamic_slice_in_dim(coulomb, row_start, tile_rows, 2)
    segment = lax.all_gather(mid_stack, "tile", axis=2, tiled=True)
    more_real, more_imag = complex_batched(coulomb_rows[0], coulomb_rows[1], segment[0], segment[1])
    return coulomb_rows.astype(jnp.float32) + jnp.stack([more_real, more_imag])


ANY = pl.BlockSpec(memory_space=pl.ANY)


def dft4(values, sign):
    (r0, i0), (r1, i1), (r2, i2), (r3, i3) = values
    er, ei, fr, fi = r0 + r2, i0 + i2, r0 - r2, i0 - i2
    gr, gi, hr, hi = r1 + r3, i1 + i3, r1 - r3, i1 - i3
    plus = (fr - hi, fi + hr)
    minus = (fr + hi, fi - hr)
    one, three = (plus, minus) if sign > 0 else (minus, plus)
    return [(er + gr, ei + gi), one, (er - gr, ei - gi), three]


def split_call(index, particle, hole, token, count, start, width):
    _, local, tile_rows, _ = particle.shape
    rows = tile_rows // count
    half = local // 2

    def kernel(index_ref, token_ref, *rest):
        ins, outs = rest[: 2 * count], rest[2 * count :]
        for shift in range(count):
            outs[shift][0] = ins[shift][...]
            outs[shift][1] = ins[count + shift][...]

    def source(shift):
        return pl.BlockSpec(
            (2, half, rows, width),
            lambda j, ix: (0, j, lax.rem(ix[0] + shift, count), start // width),
        )

    return pl.pallas_call(
        kernel,
        grid_spec=pltpu.PrefetchScalarGridSpec(
            num_scalar_prefetch=1,
            grid=(2,),
            in_specs=[ANY] + [source(shift) for shift in range(count)] * 2,
            out_specs=[pl.BlockSpec((2, 2, half, rows, width), lambda j, ix: (0, 0, j, 0, 0))]
            * count,
        ),
        out_shape=[jax.ShapeDtypeStruct((2, 2, local, rows, width), particle.dtype)] * count,
    )(index, token, *([particle] * count), *([hole] * count))


def polar_kernel(count, local, sizes):
    groups = len(sizes)
    group_of = [g for g, size in enumerate(sizes) for _ in range(size)]
    points = count * local
    quarter = points // KSIDE
    low = KSIDE
    scale = 1.0 / float(points) ** 3

    def kernel(me_ref, token_ref, *rest):
        pieces = rest[:count]
        outs = rest[count : count + count * groups]
        sc = rest[-1]
        me = me_ref[0]
        for shift in range(count):
            base = lax.rem(me + (count - shift), count) * local
            for which in range(2):
                for block in range(local // low):
                    offset = block * low
                    values = [
                        (
                            pieces[shift][which, 0, offset + n].astype(jnp.float32),
                            pieces[shift][which, 1, offset + n].astype(jnp.float32),
                        )
                        for n in range(low)
                    ]
                    for n, (real, imag) in enumerate(dft4(values, 1)):
                        sc[which, 0, base + offset + n] = real
                        sc[which, 1, base + offset + n] = imag

        def middle_digit(which, sign):
            def step(t, carry):
                first = (t // low) * (low * low) + lax.rem(t, low)
                where = [first + n * low for n in range(KSIDE)]
                values = [(sc[which, 0, w], sc[which, 1, w]) for w in where]
                for w, (real, imag) in zip(where, dft4(values, sign)):
                    sc[which, 0, w] = real
                    sc[which, 1, w] = imag
                return carry

            lax.fori_loop(0, quarter, step, 0, unroll=2)

        middle_digit(0, 1)
        middle_digit(1, 1)

        def high_digit(t, carry):
            where = [t + n * quarter for n in range(KSIDE)]
            part = dft4([(sc[0, 0, w], sc[0, 1, w]) for w in where], 1)
            hole = dft4([(sc[1, 0, w], sc[1, 1, w]) for w in where], 1)
            cells = [
                (pr * hr - pi * hi, pr * hi + pi * hr) for (pr, pi), (hr, hi) in zip(part, hole)
            ]
            for w, (real, imag) in zip(where, dft4(cells, -1)):
                sc[0, 0, w] = real
                sc[0, 1, w] = imag
            return carry

        lax.fori_loop(0, quarter, high_digit, 0, unroll=2)
        middle_digit(0, -1)
        for shift in range(count):
            base = lax.rem(me + shift, count) * local
            for block in range(local // low):
                offset = block * low
                values = [
                    (sc[0, 0, base + offset + n], sc[0, 1, base + offset + n]) for n in range(low)
                ]
                for n, (real, imag) in enumerate(dft4(values, -1)):
                    spot = offset + n
                    group = group_of[spot]
                    out = outs[shift * groups + group]
                    place = spot - sum(sizes[:group])
                    out[0, place] = (real * scale).astype(jnp.bfloat16)
                    out[1, place] = (imag * scale).astype(jnp.bfloat16)

    return kernel


def polar_call(me, token, pieces, sizes):
    count = len(pieces)
    _, _, local, rows, width = pieces[0].shape
    result = pl.pallas_call(
        polar_kernel(count, local, sizes),
        grid=(width // LANES, rows // SUB),
        in_specs=[pl.BlockSpec(memory_space=pltpu.SMEM), ANY]
        + [pl.BlockSpec((2, 2, local, SUB, LANES), lambda c, r: (0, 0, 0, r, c))] * count,
        out_specs=[
            pl.BlockSpec((2, size, SUB, LANES), lambda c, r: (0, 0, r, c)) for size in sizes
        ]
        * count,
        out_shape=[jax.ShapeDtypeStruct((2, size, rows, width), jnp.bfloat16) for size in sizes]
        * count,
        scratch_shapes=[pltpu.VMEM((2, 2, count * local, SUB, LANES), jnp.float32)],
        name="polar",
    )(me, token, *pieces)
    groups = len(sizes)
    return [[result[shift * groups + g] for shift in range(count)] for g in range(groups)]


def join_call(token, pieces):
    count = len(pieces)
    _, momenta, rows, width = pieces[0].shape
    steps = 2 if momenta % 2 == 0 else 1
    part = momenta // steps

    def kernel(token_ref, *rest):
        for n in range(count):
            rest[count][n] = rest[n][...]

    return pl.pallas_call(
        kernel,
        grid=(steps,),
        in_specs=[ANY] + [pl.BlockSpec((2, part, rows, width), lambda j: (0, j, 0, 0))] * count,
        out_specs=pl.BlockSpec((count, 2, part, rows, width), lambda j: (0, 0, j, 0, 0)),
        out_shape=jax.ShapeDtypeStruct((count,) + pieces[0].shape, pieces[0].dtype),
        name="join",
    )(token, *pieces)


def dot(left, right):
    return jnp.dot(left, right, preferred_element_type=jnp.float32)


def fill_rows(index_ref, blocks, polar, count, rows, width):
    me = index_ref[0]
    for slot, block in enumerate(blocks):
        first = index_ref[2 + slot] * (count * rows)
        for shift in range(count):
            source = lax.rem(me + (count - shift), count)
            row = pl.multiple_of(first + source * rows, rows)
            real, imag = block[shift, 0, 0], block[shift, 1, 0]
            polar[0, pl.ds(row, rows), :width] = real
            polar[0, pl.ds(row, rows), width:] = imag
            polar[1, pl.ds(row, rows), :width] = -imag
            polar[1, pl.ds(row, rows), width:] = real


def left_product(mine, polar, width):
    made = dot(mine[0], polar[0]) + dot(mine[1], polar[1])
    return made[:, :width].astype(jnp.bfloat16), made[:, width:].astype(jnp.bfloat16)


def left_call(index, token, coulomb, blocks):
    count, _, momenta, rows, width = blocks[0].shape
    points = coulomb.shape[3]
    tile_rows = count * rows

    def kernel(index_ref, rows_ref, token_ref, *rest):
        block_refs, out, polar = rest[: len(blocks)], rest[-2], rest[-1]
        fill_rows(index_ref, block_refs, polar, count, rows, width)
        out[0, 0], out[1, 0] = left_product(rows_ref[:, 0], polar, width)

    return pl.pallas_call(
        kernel,
        grid_spec=pltpu.PrefetchScalarGridSpec(
            num_scalar_prefetch=1,
            grid=(momenta,),
            in_specs=[
                pl.BlockSpec((2, 1, tile_rows, points), lambda q, ix: (0, q, ix[1], 0)),
                ANY,
            ]
            + [pl.BlockSpec((count, 2, 1, rows, width), lambda q, ix: (0, 0, q, 0, 0))]
            * len(blocks),
            out_specs=pl.BlockSpec((2, 1, tile_rows, width), lambda q, ix: (0, q, 0, 0)),
            scratch_shapes=[pltpu.VMEM((2, points, 2 * width), jnp.bfloat16)],
        ),
        out_shape=jax.ShapeDtypeStruct((2, momenta, tile_rows, width), jnp.bfloat16),
        name="left",
    )(index, coulomb, token, *blocks)


def screen_call(index, previous, coulomb, lefts, blocks, first):
    count, _, momenta, rows, width = blocks[0].shape
    points = coulomb.shape[3]
    tile_rows = count * rows
    widths = [left.shape[3] for left in lefts] + [width]
    out_shape = jax.ShapeDtypeStruct((2, coulomb.shape[1], tile_rows, points), jnp.float32)
    n_prev = 0 if previous is None else 1

    def kernel(index_ref, coulomb_ref, *rest):
        rest = rest[n_prev:]
        left_refs = rest[: len(lefts)]
        block_refs = rest[len(lefts) : len(lefts) + len(blocks)]
        out, polar, left = rest[-3], rest[-2], rest[-1]
        fill_rows(index_ref, block_refs, polar, count, rows, width)
        row = pl.multiple_of(index_ref[1] * tile_rows, tile_rows)
        mine = coulomb_ref[:, 0, pl.ds(row, tile_rows), :]
        last = [left_product(mine, polar, width)]
        column = 0
        for w, (real, imag) in zip(widths, [(ref[0, 0], ref[1, 0]) for ref in left_refs] + last):
            left[0, :, column : column + w] = real
            left[0, :, points + column : points + column + w] = -imag
            left[1, :, column : column + w] = imag
            left[1, :, points + column : points + column + w] = real
            column += w
        stacked = coulomb_ref[...].reshape(2 * points, points)
        made = dot(left[...].reshape(2 * tile_rows, 2 * points), stacked)
        out[:, 0] = mine.astype(jnp.float32) + made.reshape(2, tile_rows, points)

    return pl.pallas_call(
        kernel,
        grid_spec=pltpu.PrefetchScalarGridSpec(
            num_scalar_prefetch=1,
            grid=(momenta,),
            in_specs=[pl.BlockSpec((2, 1, points, points), lambda q, ix: (0, first + q, 0, 0))]
            + [ANY] * n_prev
            + [
                pl.BlockSpec((2, 1, tile_rows, w), lambda q, ix: (0, first + q, 0, 0))
                for w in widths[:-1]
            ]
            + [pl.BlockSpec((count, 2, 1, rows, width), lambda q, ix: (0, 0, q, 0, 0))]
            * len(blocks),
            out_specs=pl.BlockSpec(
                (2, 1, tile_rows, points), lambda q, ix: (0, first + q, 0, 0)
            ),
            scratch_shapes=[
                pltpu.VMEM((2, points, 2 * width), jnp.bfloat16),
                pltpu.VMEM((2, tile_rows, 2 * points), jnp.bfloat16),
            ],
        ),
        out_shape=out_shape,
        input_output_aliases={2: 0} if n_prev else {},
    )(index, coulomb, *([] if previous is None else [previous]), *lefts, *blocks)


def order_of(chunks, groups):
    last = chunks - 1
    order = [("split", n, 0) for n in range(min(2, chunks))]
    for n in range(chunks):
        order.append(("transform", n, 0))
        if n + 2 < chunks:
            order.append(("split", n + 2, 0))
        if n >= 2:
            order.append(("ahead", n - 2, 0))
        if n >= 1:
            order.append(("join", n - 1, 0))
        if n >= 2:
            order.append(("left", n - 2, 0))
    order += [("join", last, 0), ("ahead", last - 1, 0), ("left", last - 1, 0)]
    order += [("join", last, g) for g in range(1, groups)]
    for g in range(groups):
        order += [("ahead", last, g), ("screen", last, g)]
    return order


def pipelined(count, tiles, plan, sizes):
    chips = tiles // 2

    def exchange(pieces):
        arrived = [pieces[0]] + [None] * (count - 1)
        for shift in sorted(range(1, count), key=lambda shift: abs(2 * shift - count)):
            arrived[shift] = lax.ppermute(
                pieces[shift], "kt", [(d, (d + shift) % count) for d in range(count)]
            )
        return arrived

    def across_chips(block):
        return [block] + [
            lax.ppermute(
                block,
                "tile",
                [(t, ((t // 2 + shift) % chips) * 2 + t % 2) for t in range(tiles)],
            )
            for shift in range(1, chips)
        ]

    def across_cores(block):
        return lax.ppermute(block, "tile", [(t, t ^ 1) for t in range(tiles)])

    def body(particle, hole, coulomb):
        me = lax.axis_index("kt").astype(jnp.int32)
        tile = lax.axis_index("tile").astype(jnp.int32)
        slots = [
            lax.rem(tile // 2 + (chips - shift), chips) * 2 + (lax.rem(tile, 2) + core) % 2
            for core in range(2)
            for shift in range(chips)
        ]
        me_only = me.reshape(1)
        index = jnp.stack([me, tile] + slots).astype(jnp.int32)
        starts = [sum(plan[:n]) for n in range(len(plan))]
        last = len(plan) - 1
        everything = [coulomb.shape[1]]
        green, polar, near, over, lefts = {}, {}, {}, {}, {}

        def send_green(n, token):
            pieces = split_call(index, particle, hole, token, count, starts[n], plan[n])
            green[n] = exchange(pieces)
            return pieces[0]

        def send_polar(n, token):
            made = polar_call(me_only, token, green[n], sizes if n == last else everything)
            polar[n] = [exchange(pieces) for pieces in made]
            return made[0][0]

        def send_rows(n, g, token):
            block = join_call(token, polar[n][g])
            near[n, g] = across_chips(block)
            over[n, g] = [across_cores(block)]
            return block

        def forward_rows(n, g, token):
            for block in near[n, g][1:]:
                over[n, g].append(across_cores(block))
            return token

        def take_left(n, g, token):
            lefts[n] = left_call(index, token, coulomb, near[n, 0] + over[n, 0])
            return lefts[n]

        def screen(n, g, token):
            before = [lefts[m] for m in range(last)]
            return screen_call(
                index, token, coulomb, before, near[n, g] + over[n, g], sum(sizes[:g])
            )

        token = me_only
        steps = {"split": send_green, "transform": send_polar}
        rows_steps = {
            "join": send_rows,
            "ahead": forward_rows,
            "left": take_left,
            "screen": screen,
        }
        out = None
        for kind, n, g in order_of(len(plan), len(sizes)):
            if kind in steps:
                token = steps[kind](n, token)
            elif kind == "screen":
                out = screen(n, g, out)
            else:
                token = rows_steps[kind](n, g, token)
        return out

    return body


def solution(mesh):
    count, tiles = mesh.shape["kt"], mesh.shape["tile"]

    def sharded(body):
        return jax.shard_map(
            body,
            mesh=mesh,
            in_specs=(
                P(None, "kt", "tile", None),
                P(None, "kt", "tile", None),
                P(None, "kt", None, None),
            ),
            out_specs=P(None, "kt", "tile", None),
            check_vma=False,
        )

    def step(particle, hole, coulomb):
        _, points_k, points, _ = particle.shape
        local, tile_rows = points_k // count, points // tiles
        fits = (
            points_k == KSIDE**3
            and local % KSIDE == 0
            and tile_rows % (count * SUB) == 0
            and points % (2 * LANES) == 0
            and points >= 4 * LANES
            and tiles % 2 == 0
            and tiles > 2
        )
        if not fits:
            return sharded(generic_body)(particle, hole, coulomb)
        plan = [2 * LANES] * (points // (2 * LANES) - 1) + [LANES, LANES]
        sizes = [local - local // 4, local // 4]
        whole = sharded(pipelined(count, tiles, plan, sizes))
        return whole(particle, hole, coulomb)

    return step
```

```python
import math

import jax
import jax.numpy as jnp
from jax import lax
from jax.experimental import pallas as pl
from jax.experimental.pallas import tpu as pltpu
from jax.sharding import PartitionSpec as P


KSIDE = 4
LANES = 128
SUB = 16


HIGHEST = lax.Precision.HIGHEST


def phase_tables(points, side_count):
    point_index = jnp.arange(points, dtype=jnp.int32)
    digit_high = point_index // (side_count * side_count)
    digit_mid = point_index // side_count % side_count
    digit_low = point_index % side_count
    phase_turns = (
        digit_high[:, None] * digit_high[None, :]
        + digit_mid[:, None] * digit_mid[None, :]
        + digit_low[:, None] * digit_low[None, :]
    ) % side_count
    angles = phase_turns.astype(jnp.float32) * (2.0 * math.pi / side_count)
    return (jnp.cos(angles) / points, jnp.sin(angles) / points)


def to_cells(real_part, imag_part, cosine_table, sine_table):
    return (
        jnp.dot(cosine_table, real_part, precision=HIGHEST)
        - jnp.dot(sine_table, imag_part, precision=HIGHEST),
        jnp.dot(sine_table, real_part, precision=HIGHEST)
        + jnp.dot(cosine_table, imag_part, precision=HIGHEST),
    )


def to_momenta(real_part, imag_part, cosine_table, sine_table):
    return (
        jnp.dot(cosine_table, real_part, precision=HIGHEST)
        + jnp.dot(sine_table, imag_part, precision=HIGHEST),
        jnp.dot(cosine_table, imag_part, precision=HIGHEST)
        - jnp.dot(sine_table, real_part, precision=HIGHEST),
    )


def polarize(particle, hole_part):
    cosine_table, sine_table = phase_tables(particle.shape[1], KSIDE)
    part_real, part_imag = to_cells(
        particle[0].astype(jnp.float32), particle[1].astype(jnp.float32), cosine_table, sine_table
    )
    hole_real, hole_imag = to_cells(
        hole_part[0].astype(jnp.float32), hole_part[1].astype(jnp.float32), cosine_table, sine_table
    )
    cell_real = part_real * hole_real - part_imag * hole_imag
    cell_imag = part_real * hole_imag + part_imag * hole_real
    mom_real, mom_imag = to_momenta(cell_real, cell_imag, cosine_table, sine_table)
    return jnp.stack([mom_real, mom_imag]).astype(jnp.bfloat16)


def product_of(left_side, right_side):
    return jnp.einsum("kij,kjl->kil", left_side, right_side, preferred_element_type=jnp.float32)


def complex_batched(left_real, left_imag, right_real, right_imag):
    real_out = product_of(left_real, right_real) - product_of(left_imag, right_imag)
    imag_out = product_of(left_real, right_imag) + product_of(left_imag, right_real)
    return (real_out, imag_out)


def generic_body(green_particle, green_hole, coulomb):
    tile_rows = green_particle.shape[2]
    moved_part, moved_hole = (
        lax.all_to_all(green_particle, "kt", split_axis=3, concat_axis=1, tiled=True),
        lax.all_to_all(green_hole, "kt", split_axis=3, concat_axis=1, tiled=True),
    )
    points = moved_part.shape[1]
    narrow = moved_part.shape[3]
    polar_q = polarize(
        moved_part.reshape(2, points, tile_rows * narrow),
        moved_hole.reshape(2, points, tile_rows * narrow),
    )
    polar_q = polar_q.reshape(2, points, tile_rows, narrow)
    polar_rows = lax.all_to_all(polar_q, "kt", split_axis=1, concat_axis=3, tiled=True)
    mid_real, mid_imag = complex_batched(polar_rows[0], polar_rows[1], coulomb[0], coulomb[1])
    mid_stack = jnp.stack([mid_real.astype(jnp.bfloat16), mid_imag.astype(jnp.bfloat16)])
    row_start = lax.axis_index("tile") * tile_rows
    coulomb_rows = lax.dynamic_slice_in_dim(coulomb, row_start, tile_rows, 2)
    segment = lax.all_gather(mid_stack, "tile", axis=2, tiled=True)
    more_real, more_imag = complex_batched(coulomb_rows[0], coulomb_rows[1], segment[0], segment[1])
    return coulomb_rows.astype(jnp.float32) + jnp.stack([more_real, more_imag])


ANY = pl.BlockSpec(memory_space=pl.ANY)


def dft4(values, sign):
    (r0, i0), (r1, i1), (r2, i2), (r3, i3) = values
    er, ei, fr, fi = r0 + r2, i0 + i2, r0 - r2, i0 - i2
    gr, gi, hr, hi = r1 + r3, i1 + i3, r1 - r3, i1 - i3
    plus = (fr - hi, fi + hr)
    minus = (fr + hi, fi - hr)
    one, three = (plus, minus) if sign > 0 else (minus, plus)
    return [(er + gr, ei + gi), one, (er - gr, ei - gi), three]


def split_call(index, particle, hole, token, count, start, width):
    _, local, tile_rows, _ = particle.shape
    rows = tile_rows // count
    half = local // 2

    def kernel(index_ref, token_ref, *rest):
        ins, outs = rest[: 2 * count], rest[2 * count :]
        for shift in range(count):
            outs[shift][0] = ins[shift][...]
            outs[shift][1] = ins[count + shift][...]

    def source(shift):
        return pl.BlockSpec(
            (2, half, rows, width),
            lambda j, ix: (0, j, lax.rem(ix[0] + shift, count), start // width),
        )

    return pl.pallas_call(
        kernel,
        grid_spec=pltpu.PrefetchScalarGridSpec(
            num_scalar_prefetch=1,
            grid=(2,),
            in_specs=[ANY] + [source(shift) for shift in range(count)] * 2,
            out_specs=[pl.BlockSpec((2, 2, half, rows, width), lambda j, ix: (0, 0, j, 0, 0))]
            * count,
        ),
        out_shape=[jax.ShapeDtypeStruct((2, 2, local, rows, width), particle.dtype)] * count,
    )(index, token, *([particle] * count), *([hole] * count))


def polar_kernel(count, local):
    points = count * local
    quarter = points // KSIDE
    low = KSIDE
    scale = 1.0 / float(points) ** 3

    def kernel(me_ref, token_ref, *rest):
        pieces = rest[:count]
        outs = rest[count : 2 * count]
        sc = rest[-1]
        me = me_ref[0]
        for shift in range(count):
            base = lax.rem(me + (count - shift), count) * local
            for which in range(2):
                for block in range(local // low):
                    offset = block * low
                    values = [
                        (
                            pieces[shift][which, 0, offset + n].astype(jnp.float32),
                            pieces[shift][which, 1, offset + n].astype(jnp.float32),
                        )
                        for n in range(low)
                    ]
                    for n, (real, imag) in enumerate(dft4(values, 1)):
                        sc[which, 0, base + offset + n] = real
                        sc[which, 1, base + offset + n] = imag

        def middle_digit(which, sign):
            def step(t, carry):
                first = (t // low) * (low * low) + lax.rem(t, low)
                where = [first + n * low for n in range(KSIDE)]
                values = [(sc[which, 0, w], sc[which, 1, w]) for w in where]
                for w, (real, imag) in zip(where, dft4(values, sign)):
                    sc[which, 0, w] = real
                    sc[which, 1, w] = imag
                return carry

            lax.fori_loop(0, quarter, step, 0, unroll=2)

        middle_digit(0, 1)
        middle_digit(1, 1)

        def high_digit(t, carry):
            where = [t + n * quarter for n in range(KSIDE)]
            part = dft4([(sc[0, 0, w], sc[0, 1, w]) for w in where], 1)
            hole = dft4([(sc[1, 0, w], sc[1, 1, w]) for w in where], 1)
            cells = [
                (pr * hr - pi * hi, pr * hi + pi * hr) for (pr, pi), (hr, hi) in zip(part, hole)
            ]
            for w, (real, imag) in zip(where, dft4(cells, -1)):
                sc[0, 0, w] = real
                sc[0, 1, w] = imag
            return carry

        lax.fori_loop(0, quarter, high_digit, 0, unroll=2)
        middle_digit(0, -1)
        for shift in range(count):
            base = lax.rem(me + shift, count) * local
            for block in range(local // low):
                offset = block * low
                values = [
                    (sc[0, 0, base + offset + n], sc[0, 1, base + offset + n]) for n in range(low)
                ]
                for n, (real, imag) in enumerate(dft4(values, -1)):
                    outs[shift][0, offset + n] = (real * scale).astype(jnp.bfloat16)
                    outs[shift][1, offset + n] = (imag * scale).astype(jnp.bfloat16)

    return kernel


def polar_call(me, token, pieces):
    count = len(pieces)
    _, _, local, rows, width = pieces[0].shape
    return pl.pallas_call(
        polar_kernel(count, local),
        grid=(width // LANES, rows // SUB),
        in_specs=[pl.BlockSpec(memory_space=pltpu.SMEM), ANY]
        + [pl.BlockSpec((2, 2, local, SUB, LANES), lambda c, r: (0, 0, 0, r, c))] * count,
        out_specs=[pl.BlockSpec((2, local, SUB, LANES), lambda c, r: (0, 0, r, c))] * count,
        out_shape=[jax.ShapeDtypeStruct((2, local, rows, width), jnp.bfloat16)] * count,
        scratch_shapes=[pltpu.VMEM((2, 2, count * local, SUB, LANES), jnp.float32)],
        name="polar",
    )(me, token, *pieces)


def join_call(token, pieces, first, momenta):
    count = len(pieces)
    _, _, rows, width = pieces[0].shape
    part = math.gcd(first, momenta) if first else momenta
    part = part // 2 if part % 2 == 0 and part == momenta else part

    def kernel(token_ref, *rest):
        for n in range(count):
            rest[count][n] = rest[n][...]

    return pl.pallas_call(
        kernel,
        grid=(momenta // part,),
        in_specs=[ANY]
        + [pl.BlockSpec((2, part, rows, width), lambda j: (0, first // part + j, 0, 0))] * count,
        out_specs=pl.BlockSpec((count, 2, part, rows, width), lambda j: (0, 0, j, 0, 0)),
        out_shape=jax.ShapeDtypeStruct((count, 2, momenta, rows, width), pieces[0].dtype),
        name="join",
    )(token, *pieces)


def dot(left, right):
    return jnp.dot(left, right, preferred_element_type=jnp.float32)


def fill_rows(index_ref, blocks, q, polar, count, rows, column, width):
    me = index_ref[0]
    here, there = pl.ds(column, width), pl.ds(polar.shape[1] // 2 + column, width)
    for slot, block in enumerate(blocks):
        first = index_ref[2 + slot] * (count * rows)
        for shift in range(count):
            source = lax.rem(me + (count - shift), count)
            row = pl.multiple_of(first + source * rows, rows)
            polar[pl.ds(row, rows), here] = block[shift, 0, q]
            polar[pl.ds(row, rows), there] = block[shift, 1, q]


def left_product(mine, polar):
    _, rows, points = mine.shape
    made = dot(mine.reshape(2 * rows, points), polar[...])
    width = made.shape[1] // 2
    real = made[:rows, :width] - made[rows:, width:]
    imag = made[:rows, width:] + made[rows:, :width]
    return real.astype(jnp.bfloat16), imag.astype(jnp.bfloat16)


def left_call(index, token, coulomb, blocks):
    count, _, momenta, rows, width = blocks[0].shape
    points = coulomb.shape[3]
    tile_rows = count * rows

    each = 2 if momenta % 2 == 0 else 1

    def kernel(index_ref, rows_ref, token_ref, *rest):
        block_refs, out, polar = rest[: len(blocks)], rest[-2], rest[-1]
        for q in range(each):
            fill_rows(index_ref, block_refs, q, polar.at[q], count, rows, 0, width)
            out[0, q], out[1, q] = left_product(rows_ref[:, q], polar.at[q])

    return pl.pallas_call(
        kernel,
        grid_spec=pltpu.PrefetchScalarGridSpec(
            num_scalar_prefetch=1,
            grid=(momenta // each,),
            in_specs=[
                pl.BlockSpec((2, each, tile_rows, points), lambda q, ix: (0, q, ix[1], 0)),
                ANY,
            ]
            + [pl.BlockSpec((count, 2, each, rows, width), lambda q, ix: (0, 0, q, 0, 0))]
            * len(blocks),
            out_specs=pl.BlockSpec((2, each, tile_rows, width), lambda q, ix: (0, q, 0, 0)),
            scratch_shapes=[pltpu.VMEM((each, points, 2 * width), jnp.bfloat16)],
        ),
        out_shape=jax.ShapeDtypeStruct((2, momenta, tile_rows, width), jnp.bfloat16),
        name="left",
    )(index, coulomb, token, *blocks)


def screen_call(index, previous, coulomb, lefts, early, late, first):
    count, _, momenta, rows, late_width = late[0].shape
    early_width = early[0].shape[4]
    fresh = early_width + late_width
    points = coulomb.shape[3]
    tile_rows = count * rows
    widths = [left.shape[3] for left in lefts] + [fresh]
    out_shape = jax.ShapeDtypeStruct((2, coulomb.shape[1], tile_rows, points), jnp.float32)
    n_prev = 0 if previous is None else 1

    def kernel(index_ref, coulomb_ref, *rest):
        rest = rest[n_prev:]
        left_refs, rest = rest[: len(lefts)], rest[len(lefts) :]
        early_refs, rest = rest[: len(early)], rest[len(early) :]
        late_refs, (out, polar, left) = rest[: len(late)], rest[len(late) :]
        fill_rows(index_ref, early_refs, 0, polar, count, rows, 0, early_width)
        fill_rows(index_ref, late_refs, 0, polar, count, rows, early_width, late_width)
        row = pl.multiple_of(index_ref[1] * tile_rows, tile_rows)
        mine = coulomb_ref[:, 0, pl.ds(row, tile_rows), :]
        parts = [(ref[0, 0], ref[1, 0]) for ref in left_refs] + [left_product(mine, polar)]
        column = 0
        for w, (real, imag) in zip(widths, parts):
            left[0, :, column : column + w] = real
            left[0, :, points + column : points + column + w] = -imag
            left[1, :, column : column + w] = imag
            left[1, :, points + column : points + column + w] = real
            column += w
        stacked = coulomb_ref[...].reshape(2 * points, points)
        made = dot(left[...].reshape(2 * tile_rows, 2 * points), stacked)
        out[:, 0] = mine.astype(jnp.float32) + made.reshape(2, tile_rows, points)

    def rows_spec(width, offset):
        return pl.BlockSpec(
            (count, 2, 1, rows, width), lambda q, ix: (0, 0, offset + q, 0, 0)
        )

    return pl.pallas_call(
        kernel,
        grid_spec=pltpu.PrefetchScalarGridSpec(
            num_scalar_prefetch=1,
            grid=(momenta,),
            in_specs=[pl.BlockSpec((2, 1, points, points), lambda q, ix: (0, first + q, 0, 0))]
            + [ANY] * n_prev
            + [
                pl.BlockSpec((2, 1, tile_rows, w), lambda q, ix: (0, first + q, 0, 0))
                for w in widths[:-1]
            ]
            + [rows_spec(early_width, first)] * len(early)
            + [rows_spec(late_width, 0)] * len(late),
            out_specs=pl.BlockSpec(
                (2, 1, tile_rows, points), lambda q, ix: (0, first + q, 0, 0)
            ),
            scratch_shapes=[
                pltpu.VMEM((points, 2 * fresh), jnp.bfloat16),
                pltpu.VMEM((2, tile_rows, 2 * points), jnp.bfloat16),
            ],
        ),
        out_shape=out_shape,
        input_output_aliases={2: 0} if n_prev else {},
    )(index, coulomb, *([] if previous is None else [previous]), *lefts, *early, *late)


def order_of(chunks, groups):
    last = chunks - 1
    order = [("split", n, 0) for n in range(min(2, chunks))]
    for n in range(last):
        soon = n == last - 1
        if soon and n >= 1:
            order.append(("join", n - 1, 0))
        order.append(("transform", n, 0))
        if n + 2 < chunks:
            order.append(("split", n + 2, 0))
        if n >= 2:
            order.append(("ahead", n - 2, 0))
        if not soon and n >= 1:
            order.append(("join", n - 1, 0))
        if n >= 2:
            order.append(("left", n - 2, 0))
    order += [("transform", last, 0), ("join", last - 1, 0), ("ahead", last - 2, 0)]
    order += [("join", last, g) for g in range(groups)]
    order += [("left", last - 2, 0), ("ahead", last - 1, 0)]
    for g in range(groups):
        order += [("ahead", last, g), ("screen", last, g)]
    return order


def pipelined(count, tiles, plan, sizes):
    chips = tiles // 2

    def exchange(pieces):
        arrived = [pieces[0]] + [None] * (count - 1)
        for shift in sorted(range(1, count), key=lambda shift: abs(2 * shift - count)):
            arrived[shift] = lax.ppermute(
                pieces[shift], "kt", [(d, (d + shift) % count) for d in range(count)]
            )
        return arrived

    def across_chips(block):
        return [block] + [
            lax.ppermute(
                block,
                "tile",
                [(t, ((t // 2 + shift) % chips) * 2 + t % 2) for t in range(tiles)],
            )
            for shift in range(1, chips)
        ]

    def across_cores(block):
        return lax.ppermute(block, "tile", [(t, t ^ 1) for t in range(tiles)])

    def body(particle, hole, coulomb):
        me = lax.axis_index("kt").astype(jnp.int32)
        tile = lax.axis_index("tile").astype(jnp.int32)
        slots = [
            lax.rem(tile // 2 + (chips - shift), chips) * 2 + (lax.rem(tile, 2) + core) % 2
            for core in range(2)
            for shift in range(chips)
        ]
        me_only = me.reshape(1)
        index = jnp.stack([me, tile] + slots).astype(jnp.int32)
        starts = [sum(plan[:n]) for n in range(len(plan))]
        last = len(plan) - 1
        green, polar, near, over, lefts = {}, {}, {}, {}, {}

        def send_green(n, token):
            pieces = split_call(index, particle, hole, token, count, starts[n], plan[n])
            green[n] = exchange(pieces)
            return pieces[0]

        def send_polar(n, token):
            made = polar_call(me_only, token, green[n])
            polar[n] = exchange(made)
            return made[0]

        def send_rows(n, g, token):
            first, momenta = (sum(sizes[:g]), sizes[g]) if n == last else (0, sum(sizes))
            block = join_call(token, polar[n], first, momenta)
            near[n, g] = across_chips(block)
            over[n, g] = [across_cores(block)]
            return block

        def forward_rows(n, g, token):
            for block in near[n, g][1:]:
                over[n, g].append(across_cores(block))
            return token

        def take_left(n, g, token):
            lefts[n] = left_call(index, token, coulomb, near[n, 0] + over[n, 0])
            return lefts[n]

        def screen(n, g, token):
            before = [lefts[m] for m in range(last - 1)]
            early, late = near[n - 1, 0] + over[n - 1, 0], near[n, g] + over[n, g]
            return screen_call(index, token, coulomb, before, early, late, sum(sizes[:g]))

        token = me_only
        steps = {"split": send_green, "transform": send_polar}
        rows_steps = {
            "join": send_rows,
            "ahead": forward_rows,
            "left": take_left,
            "screen": screen,
        }
        out = None
        for kind, n, g in order_of(len(plan), len(sizes)):
            if kind in steps:
                token = steps[kind](n, token)
            elif kind == "screen":
                out = screen(n, g, out)
            else:
                token = rows_steps[kind](n, g, token)
        return out

    return body


def solution(mesh):
    count, tiles = mesh.shape["kt"], mesh.shape["tile"]

    def sharded(body):
        return jax.shard_map(
            body,
            mesh=mesh,
            in_specs=(
                P(None, "kt", "tile", None),
                P(None, "kt", "tile", None),
                P(None, "kt", None, None),
            ),
            out_specs=P(None, "kt", "tile", None),
            check_vma=False,
        )

    def step(particle, hole, coulomb):
        _, points_k, points, _ = particle.shape
        local, tile_rows = points_k // count, points // tiles
        fits = (
            points_k == KSIDE**3
            and local % KSIDE == 0
            and tile_rows % (count * SUB) == 0
            and points % (2 * LANES) == 0
            and points >= 4 * LANES
            and tiles % 2 == 0
            and tiles > 2
        )
        if not fits:
            return sharded(generic_body)(particle, hole, coulomb)
        plan = [2 * LANES] * (points // (2 * LANES) - 1) + [LANES, LANES]
        sizes = [3 * local // 8, local - 3 * local // 8] if local >= 8 else [local]
        whole = sharded(pipelined(count, tiles, plan, sizes))
        return whole(particle, hole, coulomb)

    return step
```

```python
import math

import jax
import jax.numpy as jnp
from jax import lax
from jax.experimental import pallas as pl
from jax.experimental.pallas import tpu as pltpu
from jax.sharding import PartitionSpec as P


KSIDE = 4
LANES = 128
SUB = 16


HIGHEST = lax.Precision.HIGHEST


def phase_tables(points, side_count):
    point_index = jnp.arange(points, dtype=jnp.int32)
    digit_high = point_index // (side_count * side_count)
    digit_mid = point_index // side_count % side_count
    digit_low = point_index % side_count
    phase_turns = (
        digit_high[:, None] * digit_high[None, :]
        + digit_mid[:, None] * digit_mid[None, :]
        + digit_low[:, None] * digit_low[None, :]
    ) % side_count
    angles = phase_turns.astype(jnp.float32) * (2.0 * math.pi / side_count)
    return (jnp.cos(angles) / points, jnp.sin(angles) / points)


def to_cells(real_part, imag_part, cosine_table, sine_table):
    return (
        jnp.dot(cosine_table, real_part, precision=HIGHEST)
        - jnp.dot(sine_table, imag_part, precision=HIGHEST),
        jnp.dot(sine_table, real_part, precision=HIGHEST)
        + jnp.dot(cosine_table, imag_part, precision=HIGHEST),
    )


def to_momenta(real_part, imag_part, cosine_table, sine_table):
    return (
        jnp.dot(cosine_table, real_part, precision=HIGHEST)
        + jnp.dot(sine_table, imag_part, precision=HIGHEST),
        jnp.dot(cosine_table, imag_part, precision=HIGHEST)
        - jnp.dot(sine_table, real_part, precision=HIGHEST),
    )


def polarize(particle, hole_part):
    cosine_table, sine_table = phase_tables(particle.shape[1], KSIDE)
    part_real, part_imag = to_cells(
        particle[0].astype(jnp.float32), particle[1].astype(jnp.float32), cosine_table, sine_table
    )
    hole_real, hole_imag = to_cells(
        hole_part[0].astype(jnp.float32), hole_part[1].astype(jnp.float32), cosine_table, sine_table
    )
    cell_real = part_real * hole_real - part_imag * hole_imag
    cell_imag = part_real * hole_imag + part_imag * hole_real
    mom_real, mom_imag = to_momenta(cell_real, cell_imag, cosine_table, sine_table)
    return jnp.stack([mom_real, mom_imag]).astype(jnp.bfloat16)


def product_of(left_side, right_side):
    return jnp.einsum("kij,kjl->kil", left_side, right_side, preferred_element_type=jnp.float32)


def complex_batched(left_real, left_imag, right_real, right_imag):
    real_out = product_of(left_real, right_real) - product_of(left_imag, right_imag)
    imag_out = product_of(left_real, right_imag) + product_of(left_imag, right_real)
    return (real_out, imag_out)


def generic_body(green_particle, green_hole, coulomb):
    tile_rows = green_particle.shape[2]
    moved_part, moved_hole = (
        lax.all_to_all(green_particle, "kt", split_axis=3, concat_axis=1, tiled=True),
        lax.all_to_all(green_hole, "kt", split_axis=3, concat_axis=1, tiled=True),
    )
    points = moved_part.shape[1]
    narrow = moved_part.shape[3]
    polar_q = polarize(
        moved_part.reshape(2, points, tile_rows * narrow),
        moved_hole.reshape(2, points, tile_rows * narrow),
    )
    polar_q = polar_q.reshape(2, points, tile_rows, narrow)
    polar_rows = lax.all_to_all(polar_q, "kt", split_axis=1, concat_axis=3, tiled=True)
    mid_real, mid_imag = complex_batched(polar_rows[0], polar_rows[1], coulomb[0], coulomb[1])
    mid_stack = jnp.stack([mid_real.astype(jnp.bfloat16), mid_imag.astype(jnp.bfloat16)])
    row_start = lax.axis_index("tile") * tile_rows
    coulomb_rows = lax.dynamic_slice_in_dim(coulomb, row_start, tile_rows, 2)
    segment = lax.all_gather(mid_stack, "tile", axis=2, tiled=True)
    more_real, more_imag = complex_batched(coulomb_rows[0], coulomb_rows[1], segment[0], segment[1])
    return coulomb_rows.astype(jnp.float32) + jnp.stack([more_real, more_imag])


ANY = pl.BlockSpec(memory_space=pl.ANY)


def dft4(values, sign):
    (r0, i0), (r1, i1), (r2, i2), (r3, i3) = values
    er, ei, fr, fi = r0 + r2, i0 + i2, r0 - r2, i0 - i2
    gr, gi, hr, hi = r1 + r3, i1 + i3, r1 - r3, i1 - i3
    plus = (fr - hi, fi + hr)
    minus = (fr + hi, fi - hr)
    one, three = (plus, minus) if sign > 0 else (minus, plus)
    return [(er + gr, ei + gi), one, (er - gr, ei - gi), three]


def split_call(index, particle, hole, token, count, start, width):
    _, local, tile_rows, _ = particle.shape
    rows = tile_rows // count
    half = local // 2

    def kernel(index_ref, token_ref, *rest):
        ins, outs = rest[: 2 * count], rest[2 * count :]
        for shift in range(count):
            outs[shift][0] = ins[shift][...]
            outs[shift][1] = ins[count + shift][...]

    def source(shift):
        return pl.BlockSpec(
            (2, half, rows, width),
            lambda j, ix: (0, j, lax.rem(ix[0] + shift, count), start // width),
        )

    return pl.pallas_call(
        kernel,
        grid_spec=pltpu.PrefetchScalarGridSpec(
            num_scalar_prefetch=1,
            grid=(2,),
            in_specs=[ANY] + [source(shift) for shift in range(count)] * 2,
            out_specs=[pl.BlockSpec((2, 2, half, rows, width), lambda j, ix: (0, 0, j, 0, 0))]
            * count,
        ),
        out_shape=[jax.ShapeDtypeStruct((2, 2, local, rows, width), particle.dtype)] * count,
    )(index, token, *([particle] * count), *([hole] * count))


def polar_kernel(count, local):
    points = count * local
    quarter = points // KSIDE
    low = KSIDE
    scale = 1.0 / float(points) ** 3

    def kernel(me_ref, token_ref, *rest):
        pieces = rest[:count]
        outs = rest[count : 2 * count]
        sc = rest[-1]
        me = me_ref[0]
        for shift in range(count):
            base = lax.rem(me + (count - shift), count) * local
            for which in range(2):
                for block in range(local // low):
                    offset = block * low
                    values = [
                        (
                            pieces[shift][which, 0, offset + n].astype(jnp.float32),
                            pieces[shift][which, 1, offset + n].astype(jnp.float32),
                        )
                        for n in range(low)
                    ]
                    for n, (real, imag) in enumerate(dft4(values, 1)):
                        sc[which, 0, base + offset + n] = real
                        sc[which, 1, base + offset + n] = imag

        def middle_digit(which, sign):
            def step(t, carry):
                first = (t // low) * (low * low) + lax.rem(t, low)
                where = [first + n * low for n in range(KSIDE)]
                values = [(sc[which, 0, w], sc[which, 1, w]) for w in where]
                for w, (real, imag) in zip(where, dft4(values, sign)):
                    sc[which, 0, w] = real
                    sc[which, 1, w] = imag
                return carry

            lax.fori_loop(0, quarter, step, 0, unroll=2)

        middle_digit(0, 1)
        middle_digit(1, 1)

        def high_digit(t, carry):
            where = [t + n * quarter for n in range(KSIDE)]
            part = dft4([(sc[0, 0, w], sc[0, 1, w]) for w in where], 1)
            hole = dft4([(sc[1, 0, w], sc[1, 1, w]) for w in where], 1)
            cells = [
                (pr * hr - pi * hi, pr * hi + pi * hr) for (pr, pi), (hr, hi) in zip(part, hole)
            ]
            for w, (real, imag) in zip(where, dft4(cells, -1)):
                sc[0, 0, w] = real
                sc[0, 1, w] = imag
            return carry

        lax.fori_loop(0, quarter, high_digit, 0, unroll=2)
        middle_digit(0, -1)
        for shift in range(count):
            base = lax.rem(me + shift, count) * local
            for block in range(local // low):
                offset = block * low
                values = [
                    (sc[0, 0, base + offset + n], sc[0, 1, base + offset + n]) for n in range(low)
                ]
                for n, (real, imag) in enumerate(dft4(values, -1)):
                    outs[shift][0, offset + n] = (real * scale).astype(jnp.bfloat16)
                    outs[shift][1, offset + n] = (imag * scale).astype(jnp.bfloat16)

    return kernel


def polar_call(me, token, pieces):
    count = len(pieces)
    _, _, local, rows, width = pieces[0].shape
    return pl.pallas_call(
        polar_kernel(count, local),
        grid=(width // LANES, rows // SUB),
        in_specs=[pl.BlockSpec(memory_space=pltpu.SMEM), ANY]
        + [pl.BlockSpec((2, 2, local, SUB, LANES), lambda c, r: (0, 0, 0, r, c))] * count,
        out_specs=[pl.BlockSpec((2, local, SUB, LANES), lambda c, r: (0, 0, r, c))] * count,
        out_shape=[jax.ShapeDtypeStruct((2, local, rows, width), jnp.bfloat16)] * count,
        scratch_shapes=[pltpu.VMEM((2, 2, count * local, SUB, LANES), jnp.float32)],
        name="polar",
    )(me, token, *pieces)


def join_call(token, pieces, first, momenta):
    count = len(pieces)
    _, _, rows, width = pieces[0].shape
    part = math.gcd(first, momenta) if first else momenta
    part = part // 2 if part % 2 == 0 and part == momenta else part

    def kernel(token_ref, *rest):
        for n in range(count):
            rest[count][n] = rest[n][...]

    return pl.pallas_call(
        kernel,
        grid=(momenta // part,),
        in_specs=[ANY]
        + [pl.BlockSpec((2, part, rows, width), lambda j: (0, first // part + j, 0, 0))] * count,
        out_specs=pl.BlockSpec((count, 2, part, rows, width), lambda j: (0, 0, j, 0, 0)),
        out_shape=jax.ShapeDtypeStruct((count, 2, momenta, rows, width), pieces[0].dtype),
        name="join",
    )(token, *pieces)


def dot(left, right):
    return jnp.dot(left, right, preferred_element_type=jnp.float32)


def fill_rows(index_ref, blocks, q, polar, count, rows, column, width):
    me = index_ref[0]
    here, there = pl.ds(column, width), pl.ds(polar.shape[1] // 2 + column, width)
    for slot, block in enumerate(blocks):
        first = index_ref[2 + slot] * (count * rows)
        for shift in range(count):
            source = lax.rem(me + (count - shift), count)
            row = pl.multiple_of(first + source * rows, rows)
            polar[pl.ds(row, rows), here] = block[shift, 0, q]
            polar[pl.ds(row, rows), there] = block[shift, 1, q]


def left_product(mine, polar):
    _, rows, points = mine.shape
    made = dot(mine.reshape(2 * rows, points), polar[...])
    width = made.shape[1] // 2
    real = made[:rows, :width] - made[rows:, width:]
    imag = made[:rows, width:] + made[rows:, :width]
    return real.astype(jnp.bfloat16), imag.astype(jnp.bfloat16)


def left_call(index, token, coulomb, blocks):
    count, _, momenta, rows, width = blocks[0].shape
    points = coulomb.shape[3]
    tile_rows = count * rows

    each = 2 if momenta % 2 == 0 else 1

    def kernel(index_ref, rows_ref, token_ref, *rest):
        block_refs, out, polar = rest[: len(blocks)], rest[-2], rest[-1]
        for q in range(each):
            fill_rows(index_ref, block_refs, q, polar.at[q], count, rows, 0, width)
            out[0, q], out[1, q] = left_product(rows_ref[:, q], polar.at[q])

    return pl.pallas_call(
        kernel,
        grid_spec=pltpu.PrefetchScalarGridSpec(
            num_scalar_prefetch=1,
            grid=(momenta // each,),
            in_specs=[
                pl.BlockSpec((2, each, tile_rows, points), lambda q, ix: (0, q, ix[1], 0)),
                ANY,
            ]
            + [pl.BlockSpec((count, 2, each, rows, width), lambda q, ix: (0, 0, q, 0, 0))]
            * len(blocks),
            out_specs=pl.BlockSpec((2, each, tile_rows, width), lambda q, ix: (0, q, 0, 0)),
            scratch_shapes=[pltpu.VMEM((each, points, 2 * width), jnp.bfloat16)],
        ),
        out_shape=jax.ShapeDtypeStruct((2, momenta, tile_rows, width), jnp.bfloat16),
        name="left",
    )(index, coulomb, token, *blocks)


def screen_call(index, previous, coulomb, lefts, early, late, first):
    count, _, momenta, rows, late_width = late[0].shape
    early_width = early[0].shape[4]
    fresh = early_width + late_width
    points = coulomb.shape[3]
    tile_rows = count * rows
    widths = [left.shape[3] for left in lefts] + [fresh]
    out_shape = jax.ShapeDtypeStruct((2, coulomb.shape[1], tile_rows, points), jnp.float32)
    n_prev = 0 if previous is None else 1

    def kernel(index_ref, coulomb_ref, *rest):
        rest = rest[n_prev:]
        left_refs, rest = rest[: len(lefts)], rest[len(lefts) :]
        early_refs, rest = rest[: len(early)], rest[len(early) :]
        late_refs, (out, polar, left) = rest[: len(late)], rest[len(late) :]
        fill_rows(index_ref, early_refs, 0, polar, count, rows, 0, early_width)
        fill_rows(index_ref, late_refs, 0, polar, count, rows, early_width, late_width)
        row = pl.multiple_of(index_ref[1] * tile_rows, tile_rows)
        mine = coulomb_ref[:, 0, pl.ds(row, tile_rows), :]
        parts = [(ref[0, 0], ref[1, 0]) for ref in left_refs] + [left_product(mine, polar)]
        column = 0
        for w, (real, imag) in zip(widths, parts):
            left[0, :, column : column + w] = real
            left[0, :, points + column : points + column + w] = -imag
            left[1, :, column : column + w] = imag
            left[1, :, points + column : points + column + w] = real
            column += w
        stacked = coulomb_ref[...].reshape(2 * points, points)
        made = dot(left[...].reshape(2 * tile_rows, 2 * points), stacked)
        out[:, 0] = mine.astype(jnp.float32) + made.reshape(2, tile_rows, points)

    def rows_spec(width, offset):
        return pl.BlockSpec(
            (count, 2, 1, rows, width), lambda q, ix: (0, 0, offset + q, 0, 0)
        )

    return pl.pallas_call(
        kernel,
        grid_spec=pltpu.PrefetchScalarGridSpec(
            num_scalar_prefetch=1,
            grid=(momenta,),
            in_specs=[pl.BlockSpec((2, 1, points, points), lambda q, ix: (0, first + q, 0, 0))]
            + [ANY] * n_prev
            + [
                pl.BlockSpec((2, 1, tile_rows, w), lambda q, ix: (0, first + q, 0, 0))
                for w in widths[:-1]
            ]
            + [rows_spec(early_width, first)] * len(early)
            + [rows_spec(late_width, 0)] * len(late),
            out_specs=pl.BlockSpec(
                (2, 1, tile_rows, points), lambda q, ix: (0, first + q, 0, 0)
            ),
            scratch_shapes=[
                pltpu.VMEM((points, 2 * fresh), jnp.bfloat16),
                pltpu.VMEM((2, tile_rows, 2 * points), jnp.bfloat16),
            ],
        ),
        out_shape=out_shape,
        input_output_aliases={2: 0} if n_prev else {},
    )(index, coulomb, *([] if previous is None else [previous]), *lefts, *early, *late)


def order_of(chunks, groups):
    last = chunks - 1
    order = [("split", n, 0) for n in range(min(2, chunks))]
    for n in range(last):
        soon = n == last - 1 and n >= 1
        if soon:
            order.append(("join", n - 1, 0))
        order.append(("transform", n, 0))
        late = n + 2 == last and n >= 2
        if n + 2 < chunks and not late:
            order.append(("split", n + 2, 0))
        if n >= 2:
            order.append(("ahead", n - 2, 0))
        if not soon and n >= 1:
            order.append(("join", n - 1, 0))
        if n >= 2:
            order.append(("left", n - 2, 0))
        if late:
            order.append(("split", n + 2, 0))
    order += [("transform", last, 0), ("join", last - 1, 0), ("ahead", last - 2, 0)]
    order += [("join", last, g) for g in range(groups)]
    order += [("left", last - 2, 0), ("ahead", last - 1, 0)]
    for g in range(groups):
        order += [("ahead", last, g), ("screen", last, g)]
    return order


def pipelined(count, tiles, plan, sizes):
    chips = tiles // 2

    def exchange(pieces):
        arrived = [pieces[0]] + [None] * (count - 1)
        for shift in sorted(range(1, count), key=lambda shift: abs(2 * shift - count)):
            arrived[shift] = lax.ppermute(
                pieces[shift], "kt", [(d, (d + shift) % count) for d in range(count)]
            )
        return arrived

    def across_chips(block):
        return [block] + [
            lax.ppermute(
                block,
                "tile",
                [(t, ((t // 2 + shift) % chips) * 2 + t % 2) for t in range(tiles)],
            )
            for shift in range(1, chips)
        ]

    def across_cores(block):
        return lax.ppermute(block, "tile", [(t, t ^ 1) for t in range(tiles)])

    def body(particle, hole, coulomb):
        me = lax.axis_index("kt").astype(jnp.int32)
        tile = lax.axis_index("tile").astype(jnp.int32)
        slots = [
            lax.rem(tile // 2 + (chips - shift), chips) * 2 + (lax.rem(tile, 2) + core) % 2
            for core in range(2)
            for shift in range(chips)
        ]
        me_only = me.reshape(1)
        index = jnp.stack([me, tile] + slots).astype(jnp.int32)
        starts = [sum(plan[:n]) for n in range(len(plan))]
        last = len(plan) - 1
        green, polar, near, over, lefts = {}, {}, {}, {}, {}

        def send_green(n, token):
            pieces = split_call(index, particle, hole, token, count, starts[n], plan[n])
            green[n] = exchange(pieces)
            return pieces[0]

        def send_polar(n, token):
            made = polar_call(me_only, token, green[n])
            polar[n] = exchange(made)
            return made[0]

        def send_rows(n, g, token):
            first, momenta = (sum(sizes[:g]), sizes[g]) if n == last else (0, sum(sizes))
            block = join_call(token, polar[n], first, momenta)
            near[n, g] = across_chips(block)
            over[n, g] = [across_cores(block)]
            return block

        def forward_rows(n, g, token):
            for block in near[n, g][1:]:
                over[n, g].append(across_cores(block))
            return token

        def take_left(n, g, token):
            lefts[n] = left_call(index, token, coulomb, near[n, 0] + over[n, 0])
            return lefts[n]

        def screen(n, g, token):
            before = [lefts[m] for m in range(last - 1)]
            early, late = near[n - 1, 0] + over[n - 1, 0], near[n, g] + over[n, g]
            return screen_call(index, token, coulomb, before, early, late, sum(sizes[:g]))

        token = me_only
        steps = {"split": send_green, "transform": send_polar}
        rows_steps = {
            "join": send_rows,
            "ahead": forward_rows,
            "left": take_left,
            "screen": screen,
        }
        out = None
        for kind, n, g in order_of(len(plan), len(sizes)):
            if kind in steps:
                token = steps[kind](n, token)
            elif kind == "screen":
                out = screen(n, g, out)
            else:
                token = rows_steps[kind](n, g, token)
        return out

    return body


def solution(mesh):
    count, tiles = mesh.shape["kt"], mesh.shape["tile"]

    def sharded(body):
        return jax.shard_map(
            body,
            mesh=mesh,
            in_specs=(
                P(None, "kt", "tile", None),
                P(None, "kt", "tile", None),
                P(None, "kt", None, None),
            ),
            out_specs=P(None, "kt", "tile", None),
            check_vma=False,
        )

    def step(particle, hole, coulomb):
        _, points_k, points, _ = particle.shape
        local, tile_rows = points_k // count, points // tiles
        fits = (
            points_k == KSIDE**3
            and local % KSIDE == 0
            and tile_rows % (count * SUB) == 0
            and points % (2 * LANES) == 0
            and points >= 4 * LANES
            and tiles % 2 == 0
            and tiles > 2
        )
        if not fits:
            return sharded(generic_body)(particle, hole, coulomb)
        plan = [2 * LANES] * (points // (2 * LANES) - 1) + [LANES, LANES]
        sizes = [3 * local // 8, local - 3 * local // 8] if local >= 8 else [local]
        whole = sharded(pipelined(count, tiles, plan, sizes))
        return whole(particle, hole, coulomb)

    return step
```
